32 devices in a mesh: gx: 4 (over z), gy: 4 (over y, core), af: 2 (over x).
Axes of the slice: x: 2, y: 2, z: 4, core: 2. Of those that a mesh axis runs over, the one named last changes fastest.
Arguments:
- points: bfloat16 [1024, 256], P(('gx', 'gy'), 'af'), may hold values from -12 to 12
- targets: float32 [1024, 16], P(('gx', 'gy')), may hold values from -6 to 6
Outputs:
- solution: float32 [1024, 16], P(('gx', 'gy'))
- residual: float32 [1024, 16], P(('gx', 'gy'))
The draws below stay inside these ranges and needn't reach their ends.
All inputs are finite; a program needn't handle non-finite values.
Results may differ from the reference program's by a relative error of at most 0.025.
Values may be sent and summed in bfloat16 or wider, within the bound.
A program may use at most 64 MiB of HBM per device.

```python
import jax
import jax.numpy as jnp
from jax import lax

F = 256
R = 16
P_DEV = 64
ITERS = 2
N_PTS = 1024


def draw_points(key, part):
    keys = jax.random.split(jax.random.fold_in(key, 11), 5)
    labels = jax.random.randint(keys[0], (N_PTS,), 0, 16)
    one_hot = (labels[:, None] == jnp.arange(16, dtype=jnp.int32)[None, :]).astype(jnp.float32)
    centres = 1.4 * jax.random.normal(keys[1], (16, F), jnp.float32)
    spread = jnp.exp(jax.random.uniform(keys[3], (16,), jnp.float32, 0.0, 0.47))
    noise = jax.random.normal(keys[4], (N_PTS, F), jnp.float32)
    row_centres = jnp.dot(one_hot, centres, precision=lax.Precision.HIGHEST)
    row_spread = jnp.dot(one_hot, spread, precision=lax.Precision.HIGHEST)
    values = row_centres + row_spread[:, None] * noise
    return jnp.clip(values, -12.0, 12.0).astype(jnp.bfloat16)


def block_scale(own_key, extent, pieces, smallest, high):
    factor_of, own = 1.0, jax.random.fold_in(own_key, 6)
    for dim, shards_of in pieces:
        draws = jnp.exp(jax.random.uniform(jax.random.fold_in(own, dim), (shards_of,), jnp.float32, smallest / len(pieces), high / len(pieces)))
        factor_of = factor_of * jnp.repeat(draws, extent[dim] // shards_of).reshape([-1 if axis == dim else 1 for axis in range(len(extent))])
    return factor_of


def bell_draw(own_key, dims, scale, bound, pieces=(), kind=jnp.bfloat16):
    drawn = jax.random.normal(own_key, dims, jnp.float32) * scale
    if len(pieces) > 0:
        drawn = block_scale(own_key, dims, pieces, -0.22, 0.18) * drawn
    return jnp.clip(drawn, min=-bound, max=bound).astype(kind)


def setup_inputs(seed: int = 0) -> dict:
    streams_of = jax.random.split(jax.random.key(seed), 3)
    points = draw_points(jax.random.fold_in(streams_of[2], 71), 0)
    targets = bell_draw(streams_of[1], (N_PTS, R), 1.0, 6.0, ((0, 16),), jnp.float32)
    return dict(points=points, targets=targets)


def operate(coords, norms, vector):
    lowered = lax.optimization_barrier(vector.astype(jnp.bfloat16)).astype(jnp.float32)
    scale = 0.5 / F
    blocks = coords.reshape(N_PTS // P_DEV, P_DEV, F)
    block_norms = norms.reshape(N_PTS // P_DEV, P_DEV)

    def one_block(pair):
        rows, row_norms = pair
        inner = jnp.dot(rows, coords.T)
        distance = row_norms[:, None] + norms[None, :] - 2.0 * inner
        kernel = lax.optimization_barrier(jnp.exp(-scale * distance).astype(jnp.bfloat16)).astype(jnp.float32)
        return jnp.dot(kernel, lowered)

    product = lax.map(one_block, (blocks, block_norms)).reshape(N_PTS, R)
    return product + 0.1 * vector


def reference(points, targets):
    coords = points.astype(jnp.float32)
    norms = jnp.sum(coords * coords, axis=1)
    solution = jnp.zeros_like(targets)
    residual = targets
    direction = targets
    norm_now = jnp.sum(residual * residual, axis=0)
    for step in range(ITERS):
        image = operate(coords, norms, direction)
        alpha = norm_now / jnp.sum(direction * image, axis=0)
        solution = solution + alpha * direction
        residual = residual - alpha * image
        norm_next = jnp.sum(residual * residual, axis=0)
        direction = residual + (norm_next / norm_now) * direction
        norm_now = norm_next
    return solution, residual
```

```python
import functools
import math

import jax
import jax.numpy as jnp
from jax import lax
from jax.experimental import pallas as pl
from jax.experimental.pallas import tpu as pltpu
from jax.sharding import PartitionSpec as P

ITERS = 2
MESH = pl.DeviceIdType.MESH
LANES = 128
CORES = 2


def point_norms(block):
    wide_block = block.astype(jnp.float32)
    return jnp.sum(wide_block * wide_block, axis=1)


def kernel_times(row_slab, slab_norms, col_slab, col_slab_norms, col_vector, scale):
    inner = lax.dot_general(
        row_slab, col_slab, (((1,), (1,)), ((), ())), preferred_element_type=jnp.float32
    )
    distance = slab_norms[:, None] + col_slab_norms[None, :] - 2.0 * inner
    kernel = jnp.exp(-scale * distance).astype(jnp.bfloat16)
    return jnp.dot(kernel, col_vector, preferred_element_type=jnp.float32)


def split_size(count):
    block_size = count
    while block_size > 1024 and block_size % 2 == 0:
        block_size = block_size // 2
    return block_size


def local_large(points, targets):
    whole_feat = lax.all_gather(points, "af", axis=1, tiled=True)
    norms = point_norms(whole_feat)
    half_rows = whole_feat.shape[0] // lax.axis_size("af")
    start_row = lax.axis_index("af") * half_rows
    my_points = lax.dynamic_slice_in_dim(whole_feat, start_row, half_rows, 0)
    scale = 0.5 / whole_feat.shape[1]
    stored_points = lax.all_gather(my_points, ("gx", "gy"), axis=0, tiled=True)
    stored_norms = point_norms(stored_points)

    def operate(vector):
        lowered = vector.astype(jnp.bfloat16)
        my_vector = lax.dynamic_slice_in_dim(lowered, start_row, half_rows, 0)
        empty = jnp.zeros(vector.shape, jnp.float32)
        piece = lax.all_gather(my_vector, ("gx", "gy"), axis=0, tiled=True)
        count = piece.shape[0]
        block_size = split_size(count)

        def one_block(carry, index):
            offset = index * block_size
            col_slab = lax.dynamic_slice_in_dim(stored_points, offset, block_size, 0)
            col_slab_norms = lax.dynamic_slice_in_dim(stored_norms, offset, block_size, 0)
            vector_slab = lax.dynamic_slice_in_dim(piece, offset, block_size, 0)
            return (
                carry
                + kernel_times(whole_feat, norms, col_slab, col_slab_norms, vector_slab, scale),
                None,
            )

        result, unused = lax.scan(
            one_block, empty, jnp.arange(count // block_size, dtype=jnp.int32)
        )
        return lax.psum(result, "af") + 0.1 * vector

    def two_products(values, image):
        return lax.psum(
            (jnp.sum(values * values, axis=0), jnp.sum(values * image, axis=0)), ("gx", "gy")
        )

    solution = jnp.zeros_like(targets)
    residual = targets
    image = operate(residual)
    norm_now, product = two_products(residual, image)
    alpha = norm_now / product
    direction = residual
    along = image
    for step in range(ITERS):
        solution = solution + alpha * direction
        residual = residual - alpha * along
        if step + 1 < ITERS:
            image = operate(residual)
            norm_next, product = two_products(residual, image)
            ratio = norm_next / norm_now
            alpha = norm_next / (product - ratio * norm_next / alpha)
            direction = residual + ratio * direction
            along = image + ratio * along
            norm_now = norm_next
    return (solution, residual)


def gather_and_solve(
    sizes, pts_hbm, tgt_hbm, sol_ref, res_ref, pts, tgt, kmat, stage,
    local_sem, psend, precv, tsend, trecv,
):
    nz, nw, nx = sizes
    ny = nw // CORES
    count, feats = pts_hbm.shape
    rhs = tgt_hbm.shape[0]
    z, w, x = lax.axis_index("gx"), lax.axis_index("gy"), lax.axis_index("af")
    y, c = w // CORES, w % CORES
    other = y * CORES + (1 - c)

    def shift(value, by, size):
        return lax.rem(value + by, size)

    sends = []

    def points_at(zb, wb, xb):
        rows = pl.ds(pl.multiple_of((zb * nw + wb) * count, count), count)
        return pts.at[rows, pl.ds(pl.multiple_of(xb * feats, feats), feats)]

    def points_copy(block, to, slot):
        zb, wb, xb = block
        where = points_at(zb, wb, xb)
        return pltpu.make_async_remote_copy(
            src_ref=where, dst_ref=where, send_sem=psend.at[slot],
            recv_sem=precv.at[xb, zb * nw + wb], device_id=to, device_id_type=MESH,
        )

    def targets_copy(block, to, slot):
        zb, wb = block
        where = tgt.at[zb * nw + wb]
        return pltpu.make_async_remote_copy(
            src_ref=where, dst_ref=where, send_sem=tsend.at[slot],
            recv_sem=trecv.at[zb * nw + wb], device_id=to, device_id_type=MESH,
        )

    used = {"p": 0, "t": 0}

    def send(kind, block, to):
        make = points_copy if kind == "p" else targets_copy
        copy = make(block, to, used[kind])
        used[kind] += 1
        copy.start()
        sends.append(copy)

    def arrived(kind, block):
        make = points_copy if kind == "p" else targets_copy
        make(block, (z, other, x), 0).wait_recv()

    line = [(shift(z, d, nz), w, x) for d in range(1, nz)]
    plane = [
        (dy, dx, (z, shift(y, dy, ny) * CORES + c, shift(x, dx, nx)))
        for dy in range(ny) for dx in range(nx) if dy or dx
    ]
    partner = (z, other, x)

    own_points = pltpu.make_async_copy(pts_hbm, points_at(z, w, x), local_sem.at[0])
    own_targets = pltpu.make_async_copy(tgt_hbm, tgt.at[z * nw + w], local_sem.at[1])
    own_points.start()
    own_targets.start()
    barrier = pltpu.get_barrier_semaphore()
    peers = line + [to for dy, dx, to in plane] + [partner]
    for to in peers:
        pl.semaphore_signal(barrier, inc=1, device_id=to, device_id_type=MESH)
    own_points.wait()
    own_targets.wait()
    pl.semaphore_wait(barrier, len(peers))

    def to_plane(zb):
        for dy, dx, to in plane:
            send("p", (zb, w, x), to)
            if dx == 0:
                send("t", (zb, w), to)
        send("p", (zb, w, x), partner)
        send("t", (zb, w), partner)

    for to in line:
        send("p", (z, w, x), to)
        send("t", (z, w), to)
    to_plane(z)
    for d in range(1, nz):
        zb = shift(z, d, nz)
        arrived("p", (zb, w, x))
        arrived("t", (zb, w))
        to_plane(zb)
    for d in range(nz):
        zb = shift(z, d, nz)
        for dy, dx, to in plane:
            arrived("p", (zb, to[1], to[2]))
            send("p", (zb, to[1], to[2]), partner)
            if dx == 0:
                arrived("t", (zb, to[1]))
                send("t", (zb, to[1]), partner)
    for d in range(nz):
        zb = shift(z, d, nz)
        for dy in range(ny):
            wb = shift(y, dy, ny) * CORES + (1 - c)
            for dx in range(nx):
                arrived("p", (zb, wb, shift(x, dx, nx)))
            arrived("t", (zb, wb))

    total, width = pts.shape
    factor = math.log2(math.e) / (2.0 * width)
    wide = pts[...].astype(jnp.float32)
    square = wide * wide
    high = square.astype(jnp.bfloat16)
    low = (square - high.astype(jnp.float32)).astype(jnp.bfloat16)
    ones_col = jnp.ones((width, LANES), jnp.bfloat16)
    ones_row = jnp.ones((16, width), jnp.bfloat16)
    by_row = (((1,), (1,)), ((), ()))
    norm_col = factor * (
        jnp.dot(high, ones_col, preferred_element_type=jnp.float32)
        + jnp.dot(low, ones_col, preferred_element_type=jnp.float32)
    )
    norm_row = factor * (
        lax.dot_general(ones_row, high, by_row, preferred_element_type=jnp.float32)
        + lax.dot_general(ones_row, low, by_row, preferred_element_type=jnp.float32)
    )
    block = 256
    for j in range(total // block):
        cols = slice(j * block, (j + 1) * block)
        inner = lax.dot_general(
            pts[...], pts[cols, :], by_row, preferred_element_type=jnp.float32
        )
        for k in range(block // LANES):
            at = slice(j * block + k * LANES, j * block + (k + 1) * LANES)
            power = (2.0 * factor) * inner[:, k * LANES:(k + 1) * LANES] - (
                norm_col + norm_row[0:1, at]
            )
            kmat[:, at] = jnp.exp2(power).astype(jnp.bfloat16)

    def operate(vector):
        return jnp.dot(
            vector.astype(jnp.bfloat16), kmat[...], preferred_element_type=jnp.float32
        ) + 0.1 * vector

    def over_points(values):
        return jnp.sum(values, axis=1, keepdims=True)

    residual = jnp.concatenate([tgt[g] for g in range(nz * nw)], axis=1)
    direction = residual
    solution = jnp.zeros_like(residual)
    norm_now = over_points(residual * residual)
    for step in range(ITERS):
        image = operate(direction)
        alpha = norm_now / over_points(direction * image)
        solution = solution + alpha * direction
        residual = residual - alpha * image
        if step + 1 < ITERS:
            norm_next = over_points(residual * residual)
            direction = residual + (norm_next / norm_now) * direction
            norm_now = norm_next
    own = z * nw + w
    per = LANES // count
    for index, (values, out) in enumerate(((solution, sol_ref), (residual, res_ref))):
        for k in range(total // LANES):
            stage[index, k] = values[:, k * LANES:(k + 1) * LANES]
        piece = stage[index, own // per]
        mine = piece[:, 0:count]
        for k in range(1, per):
            mine = jnp.where(own % per == k, piece[:, k * count:(k + 1) * count], mine)
        out[...] = mine
    for copy in sends:
        copy.wait_send()


def local_small(sizes, points, targets):
    nz, nw, nx = sizes
    count, feats = points.shape
    rhs = targets.shape[1]
    total, width = nz * nw * count, nx * feats
    groups = nz * nw
    ny = nw // CORES
    point_sends = (nz - 1) + nz * (ny * nx) + nz * (ny * nx - 1)
    target_sends = (nz - 1) + nz * ny + nz * (ny - 1)
    out = jax.ShapeDtypeStruct((rhs, count), jnp.float32)
    sol, res = pl.pallas_call(
        functools.partial(gather_and_solve, sizes),
        out_shape=(out, out),
        in_specs=[pl.BlockSpec(memory_space=pl.ANY)] * 2,
        out_specs=[pl.BlockSpec(memory_space=pltpu.VMEM)] * 2,
        scratch_shapes=[
            pltpu.VMEM((total, width), jnp.bfloat16),
            pltpu.VMEM((groups, rhs, count), jnp.float32),
            pltpu.VMEM((total, total), jnp.bfloat16),
            pltpu.VMEM((2, total // LANES, rhs, LANES), jnp.float32),
            pltpu.SemaphoreType.DMA((2,)),
            pltpu.SemaphoreType.DMA((point_sends,)),
            pltpu.SemaphoreType.DMA((nx, groups)),
            pltpu.SemaphoreType.DMA((target_sends,)),
            pltpu.SemaphoreType.DMA((groups,)),
        ],
        compiler_params=pltpu.CompilerParams(collective_id=0, has_side_effects=True),
    )(points, targets.T)
    return sol.T, res.T


def solution(mesh):
    sizes = tuple(mesh.shape[name] for name in ("gx", "gy", "af"))

    def local(points, targets):
        groups = sizes[0] * sizes[1]
        total = groups * points.shape[0]
        fits = 12 * total * total <= 32 * 2**20
        aligned = (
            sizes[1] % CORES == 0 and LANES % points.shape[0] == 0
            and points.shape[1] % LANES == 0 and total % 256 == 0
        )
        if fits and aligned:
            return local_small(sizes, points, targets)
        return local_large(points, targets)

    return jax.shard_map(
        local,
        mesh=mesh,
        in_specs=(P(("gx", "gy"), "af"), P(("gx", "gy"), None)),
        out_specs=(P(("gx", "gy"), None), P(("gx", "gy"), None)),
        check_vma=False,
    )
```

```python
import functools
import math

import jax
import jax.numpy as jnp
from jax import lax
from jax.experimental import pallas as pl
from jax.experimental.pallas import tpu as pltpu
from jax.sharding import PartitionSpec as P

ITERS = 2
MESH = pl.DeviceIdType.MESH
LANES = 128
CORES = 2


def point_norms(block):
    wide_block = block.astype(jnp.float32)
    return jnp.sum(wide_block * wide_block, axis=1)


def kernel_times(row_slab, slab_norms, col_slab, col_slab_norms, col_vector, scale):
    inner = lax.dot_general(
        row_slab, col_slab, (((1,), (1,)), ((), ())), preferred_element_type=jnp.float32
    )
    distance = slab_norms[:, None] + col_slab_norms[None, :] - 2.0 * inner
    kernel = jnp.exp(-scale * distance).astype(jnp.bfloat16)
    return jnp.dot(kernel, col_vector, preferred_element_type=jnp.float32)


def split_size(count):
    block_size = count
    while block_size > 1024 and block_size % 2 == 0:
        block_size = block_size // 2
    return block_size


def local_large(points, targets):
    whole_feat = lax.all_gather(points, "af", axis=1, tiled=True)
    norms = point_norms(whole_feat)
    half_rows = whole_feat.shape[0] // lax.axis_size("af")
    start_row = lax.axis_index("af") * half_rows
    my_points = lax.dynamic_slice_in_dim(whole_feat, start_row, half_rows, 0)
    scale = 0.5 / whole_feat.shape[1]
    stored_points = lax.all_gather(my_points, ("gx", "gy"), axis=0, tiled=True)
    stored_norms = point_norms(stored_points)

    def operate(vector):
        lowered = vector.astype(jnp.bfloat16)
        my_vector = lax.dynamic_slice_in_dim(lowered, start_row, half_rows, 0)
        empty = jnp.zeros(vector.shape, jnp.float32)
        piece = lax.all_gather(my_vector, ("gx", "gy"), axis=0, tiled=True)
        count = piece.shape[0]
        block_size = split_size(count)

        def one_block(carry, index):
            offset = index * block_size
            col_slab = lax.dynamic_slice_in_dim(stored_points, offset, block_size, 0)
            col_slab_norms = lax.dynamic_slice_in_dim(stored_norms, offset, block_size, 0)
            vector_slab = lax.dynamic_slice_in_dim(piece, offset, block_size, 0)
            return (
                carry
                + kernel_times(whole_feat, norms, col_slab, col_slab_norms, vector_slab, scale),
                None,
            )

        result, unused = lax.scan(
            one_block, empty, jnp.arange(count // block_size, dtype=jnp.int32)
        )
        return lax.psum(result, "af") + 0.1 * vector

    def two_products(values, image):
        return lax.psum(
            (jnp.sum(values * values, axis=0), jnp.sum(values * image, axis=0)), ("gx", "gy")
        )

    solution = jnp.zeros_like(targets)
    residual = targets
    image = operate(residual)
    norm_now, product = two_products(residual, image)
    alpha = norm_now / product
    direction = residual
    along = image
    for step in range(ITERS):
        solution = solution + alpha * direction
        residual = residual - alpha * along
        if step + 1 < ITERS:
            image = operate(residual)
            norm_next, product = two_products(residual, image)
            ratio = norm_next / norm_now
            alpha = norm_next / (product - ratio * norm_next / alpha)
            direction = residual + ratio * direction
            along = image + ratio * along
            norm_now = norm_next
    return (solution, residual)


def gather_and_solve(
    sizes, pts_hbm, tgt_hbm, base_ref, along_ref, alpha_ref, pts, tgt, kmat, norm_cols, norm_rows,
    local_sem, psend, precv, tsend, trecv,
):
    nz, nw, nx = sizes
    ny = nw // CORES
    count, feats = pts_hbm.shape
    z, w, x = lax.axis_index("gx"), lax.axis_index("gy"), lax.axis_index("af")
    y, c = w // CORES, w % CORES
    partner = (z, y * CORES + (1 - c), x)

    def points_at(d, wb, xb):
        rows = pl.ds(pl.multiple_of((d * nw + wb) * count, count), count)
        return pts.at[rows, pl.ds(pl.multiple_of(xb * feats, feats), feats)]

    def make(kind, block, to, slot, lands):
        d, wb, xb = block
        if kind == "p":
            return pltpu.make_async_remote_copy(
                src_ref=points_at(d, wb, xb), dst_ref=points_at(lands, wb, xb),
                send_sem=psend.at[slot], recv_sem=precv.at[lands, wb, xb],
                device_id=to, device_id_type=MESH,
            )
        return pltpu.make_async_remote_copy(
            src_ref=tgt.at[d * nw + wb], dst_ref=tgt.at[lands * nw + wb],
            send_sem=tsend.at[slot], recv_sem=trecv.at[lands, wb],
            device_id=to, device_id_type=MESH,
        )

    def arrived(kind, block):
        make(kind, block, partner, 0, block[0]).wait_recv()

    sends = []
    used = {"p": 0, "t": 0}

    def send(kind, block, to, lands):
        slot = used[kind]
        used[kind] += 1
        copy = make(kind, block, to, slot, lands)
        copy.start()
        sends.append(copy)

    line = [(d, (lax.rem(z + d, nz), w, x)) for d in range(1, nz)]
    plane = []
    for dy in range(ny):
        for dx in range(nx):
            if dy or dx:
                yb, xb = lax.rem(y + dy, ny), lax.rem(x + dx, nx)
                plane.append((dx, yb * CORES + c, xb))

    own_points = pltpu.make_async_copy(pts_hbm, points_at(0, w, x), local_sem.at[0])
    own_targets = pltpu.make_async_copy(tgt_hbm, tgt.at[w], local_sem.at[1])
    own_points.start()
    own_targets.start()
    barrier = pltpu.get_barrier_semaphore()
    peers = [to for d, to in line] + [(z, wb, xb) for dx, wb, xb in plane] + [partner]
    for to in peers:
        pl.semaphore_signal(barrier, inc=1, device_id=to, device_id_type=MESH)
    own_points.wait()
    own_targets.wait()
    pl.semaphore_wait(barrier, len(peers))

    def to_chip_plane(d):
        for dx, wb, xb in plane:
            send("p", (d, w, x), (z, wb, xb), d)
            if dx == 0:
                send("t", (d, w, x), (z, wb, xb), d)
        send("p", (d, w, x), partner, d)
        send("t", (d, w, x), partner, d)

    for d, to in line:
        send("p", (0, w, x), to, nz - d)
        send("t", (0, w, x), to, nz - d)
    to_chip_plane(0)
    for d in range(1, nz):
        arrived("p", (d, w, x))
        arrived("t", (d, w, x))
        to_chip_plane(d)

    def spread(d):
        for dx, wb, xb in plane:
            arrived("p", (d, wb, xb))
            send("p", (d, wb, xb), partner, d)
            if dx == 0:
                arrived("t", (d, wb, xb))
                send("t", (d, wb, xb), partner, d)

    def collect(d):
        for dy in range(ny):
            wb = lax.rem(y + dy, ny) * CORES + (1 - c)
            for dx in range(nx):
                arrived("p", (d, wb, lax.rem(x + dx, nx)))
            arrived("t", (d, wb, x))

    total, width = pts.shape
    group = total // nz
    factor = math.log2(math.e) / (2.0 * width)
    by_row = (((1,), (1,)), ((), ()))

    def make_norms(rows):
        wide = pts[rows, :].astype(jnp.float32)
        square = wide * wide
        high = square.astype(jnp.bfloat16)
        low = (square - high.astype(jnp.float32)).astype(jnp.bfloat16)
        ones_col = jnp.ones((width, LANES), jnp.bfloat16)
        ones_row = jnp.ones((16, width), jnp.bfloat16)
        norm_cols[rows, :] = factor * (
            jnp.dot(high, ones_col, preferred_element_type=jnp.float32)
            + jnp.dot(low, ones_col, preferred_element_type=jnp.float32)
        )
        norm_rows[:, rows] = factor * (
            lax.dot_general(ones_row, high, by_row, preferred_element_type=jnp.float32)
            + lax.dot_general(ones_row, low, by_row, preferred_element_type=jnp.float32)
        )

    def make_kernel(rows, cols):
        inner = lax.dot_general(
            pts[rows, :], pts[cols, :], by_row, preferred_element_type=jnp.float32
        )
        for k in range((cols.stop - cols.start) // LANES):
            at = slice(cols.start + k * LANES, cols.start + (k + 1) * LANES)
            power = (2.0 * factor) * inner[:, k * LANES:(k + 1) * LANES] - (
                norm_cols[rows, :] + norm_rows[0:1, at]
            )
            kmat[rows, at] = jnp.exp2(power).astype(jnp.bfloat16)

    for d in range(nz):
        spread(d)
    for d in range(nz):
        collect(d)
        new = slice(d * group, (d + 1) * group)
        make_norms(new)
        make_kernel(slice(0, (d + 1) * group), new)
        for e in range(d):
            make_kernel(new, slice(e * group, (e + 1) * group))

    def operate(vector):
        return jnp.dot(
            vector.astype(jnp.bfloat16), kmat[...], preferred_element_type=jnp.float32
        ) + 0.1 * vector

    def over_points(values):
        return jnp.sum(values, axis=1, keepdims=True)

    def mine(values):
        piece = values[:, 0:count]
        for k in range(1, nw):
            piece = jnp.where(w == k, values[:, k * count:(k + 1) * count], piece)
        return piece

    residual = jnp.concatenate([tgt[g] for g in range(nz * nw)], axis=1)
    direction = residual
    solution = jnp.zeros_like(residual)
    norm_now = over_points(residual * residual)
    for step in range(ITERS):
        image = operate(direction)
        alpha = norm_now / over_points(direction * image)
        if step + 1 < ITERS:
            solution = solution + alpha * direction
            residual = residual - alpha * image
            norm_next = over_points(residual * residual)
            direction = residual + (norm_next / norm_now) * direction
            norm_now = norm_next
    base_ref[0] = mine(solution)
    base_ref[1] = mine(residual)
    along_ref[0] = mine(direction)
    along_ref[1] = mine(image)
    alpha_ref[...] = jnp.broadcast_to(alpha, alpha_ref.shape)

    for copy in sends:
        copy.wait_send()


def local_small(sizes, points, targets):
    nz, nw, nx = sizes
    count, feats = points.shape
    rhs = targets.shape[1]
    total, width = nz * nw * count, nx * feats
    groups = nz * nw
    ny = nw // CORES
    most_sends = 2 * nz * nw * nx + CORES * nz * ny * nx
    base, along, alpha = pl.pallas_call(
        functools.partial(gather_and_solve, sizes),
        out_shape=(
            pltpu.VMEM((2, rhs, count), jnp.float32),
            pltpu.VMEM((2, rhs, count), jnp.float32),
            pltpu.VMEM((rhs, count), jnp.float32),
        ),
        in_specs=[pl.BlockSpec(memory_space=pl.ANY)] * 2,
        out_specs=[pl.BlockSpec(memory_space=pltpu.VMEM)] * 3,
        scratch_shapes=[
            pltpu.VMEM((total, width), jnp.bfloat16),
            pltpu.VMEM((groups, rhs, count), jnp.float32),
            pltpu.VMEM((total, total), jnp.bfloat16),
            pltpu.VMEM((total, LANES), jnp.float32),
            pltpu.VMEM((16, total), jnp.float32),
            pltpu.SemaphoreType.DMA((2,)),
            pltpu.SemaphoreType.DMA((most_sends,)),
            pltpu.SemaphoreType.DMA((nz, nw, nx)),
            pltpu.SemaphoreType.DMA((most_sends,)),
            pltpu.SemaphoreType.DMA((nz, nw)),
        ],
        compiler_params=pltpu.CompilerParams(collective_id=0, has_side_effects=True),
    )(points, targets.T)
    last = base[0] + alpha * along[0]
    left = base[1] - alpha * along[1]
    return last.T, left.T


def solution(mesh):
    sizes = tuple(mesh.shape[name] for name in ("gx", "gy", "af"))

    def local(points, targets):
        groups = sizes[0] * sizes[1]
        total = groups * points.shape[0]
        fits = 12 * total * total <= 32 * 2**20
        aligned = (
            sizes[1] % CORES == 0 and LANES % points.shape[0] == 0
            and points.shape[1] % LANES == 0 and total % 256 == 0
        )
        if fits and aligned:
            return local_small(sizes, points, targets)
        return local_large(points, targets)

    return jax.shard_map(
        local,
        mesh=mesh,
        in_specs=(P(("gx", "gy"), "af"), P(("gx", "gy"), None)),
        out_specs=(P(("gx", "gy"), None), P(("gx", "gy"), None)),
        check_vma=False,
    )
```

```python
import functools
import math

import jax
import jax.numpy as jnp
from jax import lax
from jax.experimental import pallas as pl
from jax.experimental.pallas import tpu as pltpu
from jax.sharding import PartitionSpec as P

ITERS = 2
MESH = pl.DeviceIdType.MESH
LANES = 128
CORES = 2


def point_norms(block):
    wide_block = block.astype(jnp.float32)
    return jnp.sum(wide_block * wide_block, axis=1)


def kernel_times(row_slab, slab_norms, col_slab, col_slab_norms, col_vector, scale):
    inner = lax.dot_general(
        row_slab, col_slab, (((1,), (1,)), ((), ())), preferred_element_type=jnp.float32
    )
    distance = slab_norms[:, None] + col_slab_norms[None, :] - 2.0 * inner
    kernel = jnp.exp(-scale * distance).astype(jnp.bfloat16)
    return jnp.dot(kernel, col_vector, preferred_element_type=jnp.float32)


def split_size(count):
    block_size = count
    while block_size > 1024 and block_size % 2 == 0:
        block_size = block_size // 2
    return block_size


def local_large(points, targets):
    whole_feat = lax.all_gather(points, "af", axis=1, tiled=True)
    norms = point_norms(whole_feat)
    half_rows = whole_feat.shape[0] // lax.axis_size("af")
    start_row = lax.axis_index("af") * half_rows
    my_points = lax.dynamic_slice_in_dim(whole_feat, start_row, half_rows, 0)
    scale = 0.5 / whole_feat.shape[1]
    stored_points = lax.all_gather(my_points, ("gx", "gy"), axis=0, tiled=True)
    stored_norms = point_norms(stored_points)

    def operate(vector):
        lowered = vector.astype(jnp.bfloat16)
        my_vector = lax.dynamic_slice_in_dim(lowered, start_row, half_rows, 0)
        empty = jnp.zeros(vector.shape, jnp.float32)
        piece = lax.all_gather(my_vector, ("gx", "gy"), axis=0, tiled=True)
        count = piece.shape[0]
        block_size = split_size(count)

        def one_block(carry, index):
            offset = index * block_size
            col_slab = lax.dynamic_slice_in_dim(stored_points, offset, block_size, 0)
            col_slab_norms = lax.dynamic_slice_in_dim(stored_norms, offset, block_size, 0)
            vector_slab = lax.dynamic_slice_in_dim(piece, offset, block_size, 0)
            return (
                carry
                + kernel_times(whole_feat, norms, col_slab, col_slab_norms, vector_slab, scale),
                None,
            )

        result, unused = lax.scan(
            one_block, empty, jnp.arange(count // block_size, dtype=jnp.int32)
        )
        return lax.psum(result, "af") + 0.1 * vector

    def two_products(values, image):
        return lax.psum(
            (jnp.sum(values * values, axis=0), jnp.sum(values * image, axis=0)), ("gx", "gy")
        )

    solution = jnp.zeros_like(targets)
    residual = targets
    image = operate(residual)
    norm_now, product = two_products(residual, image)
    alpha = norm_now / product
    direction = residual
    along = image
    for step in range(ITERS):
        solution = solution + alpha * direction
        residual = residual - alpha * along
        if step + 1 < ITERS:
            image = operate(residual)
            norm_next, product = two_products(residual, image)
            ratio = norm_next / norm_now
            alpha = norm_next / (product - ratio * norm_next / alpha)
            direction = residual + ratio * direction
            along = image + ratio * along
            norm_now = norm_next
    return (solution, residual)


def gather_and_solve(
    sizes, pts_hbm, tgt_hbm, base_ref, along_ref, alpha_ref, pts, tgt, kmat,
    local_sem, psend, precv, tsend, trecv,
):
    nz, nw, nx = sizes
    ny = nw // CORES
    count, feats = pts_hbm.shape
    rhs = tgt_hbm.shape[0]
    z, w, x = lax.axis_index("gx"), lax.axis_index("gy"), lax.axis_index("af")
    y, c = w // CORES, w % CORES
    other = y * CORES + (1 - c)

    def shift(value, by, size):
        return lax.rem(value + by, size)

    sends = []

    def points_at(zb, wb, xb):
        rows = pl.ds(pl.multiple_of((zb * nw + wb) * count, count), count)
        return pts.at[rows, pl.ds(pl.multiple_of(xb * feats, feats), feats)]

    def points_copy(block, to, slot):
        zb, wb, xb = block
        where = points_at(zb, wb, xb)
        return pltpu.make_async_remote_copy(
            src_ref=where, dst_ref=where, send_sem=psend.at[slot],
            recv_sem=precv.at[xb, zb * nw + wb], device_id=to, device_id_type=MESH,
        )

    def targets_copy(block, to, slot):
        zb, wb = block
        where = tgt.at[zb * nw + wb]
        return pltpu.make_async_remote_copy(
            src_ref=where, dst_ref=where, send_sem=tsend.at[slot],
            recv_sem=trecv.at[zb * nw + wb], device_id=to, device_id_type=MESH,
        )

    used = {"p": 0, "t": 0}

    def send(kind, block, to):
        make = points_copy if kind == "p" else targets_copy
        copy = make(block, to, used[kind])
        used[kind] += 1
        copy.start()
        sends.append(copy)

    def arrived(kind, block):
        make = points_copy if kind == "p" else targets_copy
        make(block, (z, other, x), 0).wait_recv()

    line = [(shift(z, d, nz), w, x) for d in range(1, nz)]
    plane = [
        (dy, dx, (z, shift(y, dy, ny) * CORES + c, shift(x, dx, nx)))
        for dy in range(ny) for dx in range(nx) if dy or dx
    ]
    partner = (z, other, x)

    own_points = pltpu.make_async_copy(pts_hbm, points_at(z, w, x), local_sem.at[0])
    own_targets = pltpu.make_async_copy(tgt_hbm, tgt.at[z * nw + w], local_sem.at[1])
    own_points.start()
    own_targets.start()
    barrier = pltpu.get_barrier_semaphore()
    peers = line + [to for dy, dx, to in plane] + [partner]
    for to in peers:
        pl.semaphore_signal(barrier, inc=1, device_id=to, device_id_type=MESH)
    own_points.wait()
    own_targets.wait()
    pl.semaphore_wait(barrier, len(peers))

    def to_plane(zb):
        for dy, dx, to in plane:
            send("p", (zb, w, x), to)
            if dx == 0:
                send("t", (zb, w), to)
        send("p", (zb, w, x), partner)
        send("t", (zb, w), partner)

    for to in line:
        send("p", (z, w, x), to)
        send("t", (z, w), to)
    to_plane(z)
    for d in range(1, nz):
        zb = shift(z, d, nz)
        arrived("p", (zb, w, x))
        arrived("t", (zb, w))
        to_plane(zb)
    for d in range(nz):
        zb = shift(z, d, nz)
        for dy, dx, to in plane:
            arrived("p", (zb, to[1], to[2]))
            send("p", (zb, to[1], to[2]), partner)
            if dx == 0:
                arrived("t", (zb, to[1]))
                send("t", (zb, to[1]), partner)
    for d in range(nz):
        zb = shift(z, d, nz)
        for dy in range(ny):
            wb = shift(y, dy, ny) * CORES + (1 - c)
            for dx in range(nx):
                arrived("p", (zb, wb, shift(x, dx, nx)))
            arrived("t", (zb, wb))

    total, width = pts.shape
    factor = math.log2(math.e) / (2.0 * width)
    wide = pts[...].astype(jnp.float32)
    square = wide * wide
    high = square.astype(jnp.bfloat16)
    low = (square - high.astype(jnp.float32)).astype(jnp.bfloat16)
    ones_col = jnp.ones((width, LANES), jnp.bfloat16)
    ones_row = jnp.ones((16, width), jnp.bfloat16)
    by_row = (((1,), (1,)), ((), ()))
    norm_col = factor * (
        jnp.dot(high, ones_col, preferred_element_type=jnp.float32)
        + jnp.dot(low, ones_col, preferred_element_type=jnp.float32)
    )
    norm_row = factor * (
        lax.dot_general(ones_row, high, by_row, preferred_element_type=jnp.float32)
        + lax.dot_general(ones_row, low, by_row, preferred_element_type=jnp.float32)
    )
    block = 256
    for j in range(total // block):
        cols = slice(j * block, (j + 1) * block)
        inner = lax.dot_general(
            pts[...], pts[cols, :], by_row, preferred_element_type=jnp.float32
        )
        for k in range(block // LANES):
            at = slice(j * block + k * LANES, j * block + (k + 1) * LANES)
            power = (2.0 * factor) * inner[:, k * LANES:(k + 1) * LANES] - (
                norm_col + norm_row[0:1, at]
            )
            kmat[:, at] = jnp.exp2(power).astype(jnp.bfloat16)

    def operate(vector):
        return jnp.dot(
            vector.astype(jnp.bfloat16), kmat[...], preferred_element_type=jnp.float32
        ) + 0.1 * vector

    def over_points(values):
        return jnp.sum(values, axis=1, keepdims=True)

    residual = jnp.concatenate([tgt[g] for g in range(nz * nw)], axis=1)
    direction = residual
    solution = jnp.zeros_like(residual)
    norm_now = over_points(residual * residual)
    for step in range(ITERS):
        image = operate(direction)
        alpha = norm_now / over_points(direction * image)
        if step + 1 < ITERS:
            solution = solution + alpha * direction
            residual = residual - alpha * image
            norm_next = over_points(residual * residual)
            direction = residual + (norm_next / norm_now) * direction
            norm_now = norm_next

    def mine(values):
        per = LANES // count
        own = z * nw + w
        piece = values[:, 0:LANES]
        for k in range(1, total // LANES):
            piece = jnp.where(own // per == k, values[:, k * LANES:(k + 1) * LANES], piece)
        part = piece[:, 0:count]
        for k in range(1, per):
            part = jnp.where(own % per == k, piece[:, k * count:(k + 1) * count], part)
        return part

    base_ref[0] = mine(solution)
    base_ref[1] = mine(residual)
    along_ref[0] = mine(direction)
    along_ref[1] = mine(image)
    alpha_ref[...] = jnp.broadcast_to(alpha, alpha_ref.shape)
    for copy in sends:
        copy.wait_send()


def local_small(sizes, points, targets):
    nz, nw, nx = sizes
    count, feats = points.shape
    rhs = targets.shape[1]
    total, width = nz * nw * count, nx * feats
    groups = nz * nw
    ny = nw // CORES
    point_sends = (nz - 1) + nz * (ny * nx) + nz * (ny * nx - 1)
    target_sends = (nz - 1) + nz * ny + nz * (ny - 1)
    base, along, alpha = pl.pallas_call(
        functools.partial(gather_and_solve, sizes),
        out_shape=(
            pltpu.VMEM((2, rhs, count), jnp.float32),
            pltpu.VMEM((2, rhs, count), jnp.float32),
            pltpu.VMEM((rhs, count), jnp.float32),
        ),
        in_specs=[pl.BlockSpec(memory_space=pl.ANY)] * 2,
        out_specs=[pl.BlockSpec(memory_space=pltpu.VMEM)] * 3,
        scratch_shapes=[
            pltpu.VMEM((total, width), jnp.bfloat16),
            pltpu.VMEM((groups, rhs, count), jnp.float32),
            pltpu.VMEM((total, total), jnp.bfloat16),
            pltpu.SemaphoreType.DMA((2,)),
            pltpu.SemaphoreType.DMA((point_sends,)),
            pltpu.SemaphoreType.DMA((nx, groups)),
            pltpu.SemaphoreType.DMA((target_sends,)),
            pltpu.SemaphoreType.DMA((groups,)),
        ],
        compiler_params=pltpu.CompilerParams(collective_id=0, has_side_effects=True),
    )(points, targets.T)
    last = base[0] + alpha * along[0]
    left = base[1] - alpha * along[1]
    return last.T, left.T


def solution(mesh):
    sizes = tuple(mesh.shape[name] for name in ("gx", "gy", "af"))

    def local(points, targets):
        groups = sizes[0] * sizes[1]
        total = groups * points.shape[0]
        fits = 12 * total * total <= 32 * 2**20
        aligned = (
            sizes[1] % CORES == 0 and LANES % points.shape[0] == 0
            and points.shape[1] % LANES == 0 and total % 256 == 0
        )
        if fits and aligned:
            return local_small(sizes, points, targets)
        return local_large(points, targets)

    return jax.shard_map(
        local,
        mesh=mesh,
        in_specs=(P(("gx", "gy"), "af"), P(("gx", "gy"), None)),
        out_specs=(P(("gx", "gy"), None), P(("gx", "gy"), None)),
        check_vma=False,
    )
```

```python
import functools
import math

import jax
import jax.numpy as jnp
from jax import lax
from jax.experimental import pallas as pl
from jax.experimental.pallas import tpu as pltpu
from jax.sharding import PartitionSpec as P

ITERS = 2
MESH = pl.DeviceIdType.MESH
LANES = 128
CORES = 2


def point_norms(block):
    wide_block = block.astype(jnp.float32)
    return jnp.sum(wide_block * wide_block, axis=1)


def kernel_times(row_slab, slab_norms, col_slab, col_slab_norms, col_vector, scale):
    inner = lax.dot_general(
        row_slab, col_slab, (((1,), (1,)), ((), ())), preferred_element_type=jnp.float32
    )
    distance = slab_norms[:, None] + col_slab_norms[None, :] - 2.0 * inner
    kernel = jnp.exp(-scale * distance).astype(jnp.bfloat16)
    return jnp.dot(kernel, col_vector, preferred_element_type=jnp.float32)


def split_size(count):
    block_size = count
    while block_size > 1024 and block_size % 2 == 0:
        block_size = block_size // 2
    return block_size


def local_large(points, targets):
    whole_feat = lax.all_gather(points, "af", axis=1, tiled=True)
    norms = point_norms(whole_feat)
    half_rows = whole_feat.shape[0] // lax.axis_size("af")
    start_row = lax.axis_index("af") * half_rows
    my_points = lax.dynamic_slice_in_dim(whole_feat, start_row, half_rows, 0)
    scale = 0.5 / whole_feat.shape[1]
    stored_points = lax.all_gather(my_points, ("gx", "gy"), axis=0, tiled=True)
    stored_norms = point_norms(stored_points)

    def operate(vector):
        lowered = vector.astype(jnp.bfloat16)
        my_vector = lax.dynamic_slice_in_dim(lowered, start_row, half_rows, 0)
        empty = jnp.zeros(vector.shape, jnp.float32)
        piece = lax.all_gather(my_vector, ("gx", "gy"), axis=0, tiled=True)
        count = piece.shape[0]
        block_size = split_size(count)

        def one_block(carry, index):
            offset = index * block_size
            col_slab = lax.dynamic_slice_in_dim(stored_points, offset, block_size, 0)
            col_slab_norms = lax.dynamic_slice_in_dim(stored_norms, offset, block_size, 0)
            vector_slab = lax.dynamic_slice_in_dim(piece, offset, block_size, 0)
            return (
                carry
                + kernel_times(whole_feat, norms, col_slab, col_slab_norms, vector_slab, scale),
                None,
            )

        result, unused = lax.scan(
            one_block, empty, jnp.arange(count // block_size, dtype=jnp.int32)
        )
        return lax.psum(result, "af") + 0.1 * vector

    def two_products(values, image):
        return lax.psum(
            (jnp.sum(values * values, axis=0), jnp.sum(values * image, axis=0)), ("gx", "gy")
        )

    solution = jnp.zeros_like(targets)
    residual = targets
    image = operate(residual)
    norm_now, product = two_products(residual, image)
    alpha = norm_now / product
    direction = residual
    along = image
    for step in range(ITERS):
        solution = solution + alpha * direction
        residual = residual - alpha * along
        if step + 1 < ITERS:
            image = operate(residual)
            norm_next, product = two_products(residual, image)
            ratio = norm_next / norm_now
            alpha = norm_next / (product - ratio * norm_next / alpha)
            direction = residual + ratio * direction
            along = image + ratio * along
            norm_now = norm_next
    return (solution, residual)


def gather_and_solve(
    sizes, pts_hbm, tgt_hbm, base_ref, along_ref, alpha_ref, pts, tgt, kmat,
    local_sem, send_sem, line_sem, plane_sem, side_sem, partner_sem,
):
    nz, nw, nx = sizes
    ny = nw // CORES
    count, feats = pts_hbm.shape
    rhs = tgt_hbm.shape[0]
    z, w, x = lax.axis_index("gx"), lax.axis_index("gy"), lax.axis_index("af")
    y, c = w // CORES, w % CORES
    other = y * CORES + (1 - c)

    def shift(value, by, size):
        return lax.rem(value + by, size)

    def points_at(zb, wb, xb):
        rows = pl.ds(pl.multiple_of((zb * nw + wb) * count, count), count)
        return pts.at[rows, pl.ds(pl.multiple_of(xb * feats, feats), feats)]

    def part(kind, block):
        zb, wb, xb = block
        return points_at(zb, wb, xb) if kind == 0 else tgt.at[zb * nw + wb]

    def make(kind, block, to, recv_sem):
        where = part(kind, block)
        return pltpu.make_async_remote_copy(
            src_ref=where, dst_ref=where, send_sem=send_sem.at[kind],
            recv_sem=recv_sem, device_id=to, device_id_type=MESH,
        )

    sent = [0, 0]

    def send(kind, block, to, recv_sem):
        make(kind, block, to, recv_sem).start()
        sent[kind] += 1

    def arrived(kind, block, recv_sem):
        make(kind, block, (z, other, x), recv_sem).wait_recv()

    def in_plane(kind, d, dy, dx):
        return plane_sem.at[d, dy, dx] if kind == 0 else side_sem.at[d, dy]

    line = [(d, (shift(z, d, nz), w, x)) for d in range(1, nz)]
    plane = [
        (dy, dx, (z, shift(y, dy, ny) * CORES + c, shift(x, dx, nx)))
        for dy in range(ny) for dx in range(nx) if dy or dx
    ]
    partner = (z, other, x)

    own_points = pltpu.make_async_copy(pts_hbm, points_at(z, w, x), local_sem.at[0])
    own_targets = pltpu.make_async_copy(tgt_hbm, tgt.at[z * nw + w], local_sem.at[1])
    own_points.start()
    own_targets.start()
    barrier = pltpu.get_barrier_semaphore()
    peers = [to for d, to in line] + [to for dy, dx, to in plane] + [partner]
    for to in peers:
        pl.semaphore_signal(barrier, inc=1, device_id=to, device_id_type=MESH)
    own_points.wait()
    own_targets.wait()
    pl.semaphore_wait(barrier, len(peers))

    def to_plane(d):
        zb = shift(z, d, nz)
        for dy, dx, to in plane:
            back_y, back_x = (ny - dy) % ny, (nx - dx) % nx
            send(0, (zb, w, x), to, in_plane(0, d, back_y, back_x))
            if dx == 0:
                send(1, (zb, w, x), to, in_plane(1, d, back_y, back_x))
        for kind in range(2):
            send(kind, (zb, w, x), partner, partner_sem.at[kind])

    for d, to in line:
        for kind in range(2):
            send(kind, (z, w, x), to, line_sem.at[kind, nz - d])
    to_plane(0)
    for d in range(1, nz):
        for kind in range(2):
            arrived(kind, (shift(z, d, nz), w, x), line_sem.at[kind, d])
        to_plane(d)
    for d in range(nz):
        for dy, dx, to in plane:
            block = (shift(z, d, nz), to[1], to[2])
            for kind in range(2 if dx == 0 else 1):
                arrived(kind, block, in_plane(kind, d, dy, dx))
                send(kind, block, partner, partner_sem.at[kind])

    def all_of(kind, blocks):
        return pts.at[0:blocks * count // nx] if kind == 0 else tgt.at[0:blocks]

    def of_bytes(kind, blocks):
        where = all_of(kind, blocks)
        return pltpu.make_async_remote_copy(
            src_ref=where, dst_ref=where, send_sem=send_sem.at[kind],
            recv_sem=partner_sem.at[kind], device_id=partner, device_id_type=MESH,
        )

    of_bytes(0, nz * ny * nx).wait_recv()
    of_bytes(1, nz * ny).wait_recv()

    total, width = pts.shape
    factor = math.log2(math.e) / (2.0 * width)
    wide = pts[...].astype(jnp.float32)
    square = wide * wide
    high = square.astype(jnp.bfloat16)
    low = (square - high.astype(jnp.float32)).astype(jnp.bfloat16)
    ones_col = jnp.ones((width, LANES), jnp.bfloat16)
    ones_row = jnp.ones((16, width), jnp.bfloat16)
    by_row = (((1,), (1,)), ((), ()))
    norm_col = factor * (
        jnp.dot(high, ones_col, preferred_element_type=jnp.float32)
        + jnp.dot(low, ones_col, preferred_element_type=jnp.float32)
    )
    norm_row = factor * (
        lax.dot_general(ones_row, high, by_row, preferred_element_type=jnp.float32)
        + lax.dot_general(ones_row, low, by_row, preferred_element_type=jnp.float32)
    )
    block = 256
    for j in range(total // block):
        cols = slice(j * block, (j + 1) * block)
        inner = lax.dot_general(
            pts[...], pts[cols, :], by_row, preferred_element_type=jnp.float32
        )
        for k in range(block // LANES):
            at = slice(j * block + k * LANES, j * block + (k + 1) * LANES)
            power = (2.0 * factor) * inner[:, k * LANES:(k + 1) * LANES] - (
                norm_col + norm_row[0:1, at]
            )
            kmat[:, at] = jnp.exp2(power).astype(jnp.bfloat16)

    def operate(vector):
        return jnp.dot(
            vector.astype(jnp.bfloat16), kmat[...], preferred_element_type=jnp.float32
        ) + 0.1 * vector

    def over_points(values):
        return jnp.sum(values, axis=1, keepdims=True)

    residual = jnp.concatenate([tgt[g] for g in range(nz * nw)], axis=1)
    direction = residual
    solution = jnp.zeros_like(residual)
    norm_now = over_points(residual * residual)
    for step in range(ITERS):
        image = operate(direction)
        alpha = norm_now / over_points(direction * image)
        if step + 1 < ITERS:
            solution = solution + alpha * direction
            residual = residual - alpha * image
            norm_next = over_points(residual * residual)
            direction = residual + (norm_next / norm_now) * direction
            norm_now = norm_next

    def mine(values):
        per = LANES // count
        own = z * nw + w
        piece = values[:, 0:LANES]
        for k in range(1, total // LANES):
            piece = jnp.where(own // per == k, values[:, k * LANES:(k + 1) * LANES], piece)
        part = piece[:, 0:count]
        for k in range(1, per):
            part = jnp.where(own % per == k, piece[:, k * count:(k + 1) * count], part)
        return part

    base_ref[0] = mine(solution)
    base_ref[1] = mine(residual)
    along_ref[0] = mine(direction)
    along_ref[1] = mine(image)
    alpha_ref[...] = jnp.broadcast_to(alpha, alpha_ref.shape)
    for kind in range(2):
        of_bytes(kind, sent[kind]).wait_send()


def local_small(sizes, points, targets):
    nz, nw, nx = sizes
    count, feats = points.shape
    rhs = targets.shape[1]
    total, width = nz * nw * count, nx * feats
    groups = nz * nw
    ny = nw // CORES
    base, along, alpha = pl.pallas_call(
        functools.partial(gather_and_solve, sizes),
        out_shape=(
            pltpu.VMEM((2, rhs, count), jnp.float32),
            pltpu.VMEM((2, rhs, count), jnp.float32),
            pltpu.VMEM((rhs, count), jnp.float32),
        ),
        in_specs=[pl.BlockSpec(memory_space=pl.ANY)] * 2,
        out_specs=[pl.BlockSpec(memory_space=pltpu.VMEM)] * 3,
        scratch_shapes=[
            pltpu.VMEM((total, width), jnp.bfloat16),
            pltpu.VMEM((groups, rhs, count), jnp.float32),
            pltpu.VMEM((total, total), jnp.bfloat16),
            pltpu.SemaphoreType.DMA((2,)),
            pltpu.SemaphoreType.DMA((2,)),
            pltpu.SemaphoreType.DMA((2, nz)),
            pltpu.SemaphoreType.DMA((nz, ny, nx)),
            pltpu.SemaphoreType.DMA((nz, ny)),
            pltpu.SemaphoreType.DMA((2,)),
        ],
        compiler_params=pltpu.CompilerParams(collective_id=0, has_side_effects=True),
    )(points, targets.T)
    last = base[0] + alpha * along[0]
    left = base[1] - alpha * along[1]
    return last.T, left.T


def solution(mesh):
    sizes = tuple(mesh.shape[name] for name in ("gx", "gy", "af"))

    def local(points, targets):
        groups = sizes[0] * sizes[1]
        total = groups * points.shape[0]
        fits = 12 * total * total <= 32 * 2**20
        aligned = (
            sizes[1] % CORES == 0 and LANES % points.shape[0] == 0
            and points.shape[1] % LANES == 0 and total % 256 == 0
        )
        if fits and aligned:
            return local_small(sizes, points, targets)
        return local_large(points, targets)

    return jax.shard_map(
        local,
        mesh=mesh,
        in_specs=(P(("gx", "gy"), "af"), P(("gx", "gy"), None)),
        out_specs=(P(("gx", "gy"), None), P(("gx", "gy"), None)),
        check_vma=False,
    )
```
